16 devices in a mesh: prob: 2 (over y, z), feat: 8 (over x, core).
Axes of the slice: x: 4, y: 2, z: 1, core: 2. Of those that a mesh axis runs over, the one named last changes fastest.
The devices are a block of a 4x4x8 slice.
Arguments:
- x_data: bfloat16 [8192, 784], P('prob'), parts along dimension 0
- targets: float32 [8192], P('prob'), parts along dimension 0
- w_in: float32 [1024, 784], P(('prob', 'feat')), parts along dimension 0
- w_out: float32 [1024], P(('prob', 'feat')), parts along dimension 0
- reg_weight: float32 [2], P('prob'), parts along dimension 0
- step_size: float32 [2], P('prob'), parts along dimension 0
Outputs:
- output 1: float32 [1024, 784], P(('prob', 'feat')), parts along dimension 0
- output 2: float32 [1024], P(('prob', 'feat')), parts along dimension 0
- output 3: float32 [12], P('prob'), parts along dimension 0
There are 2 independent parts. The reference program is written for one: setup_inputs(seed, part) draws one part's arguments, and reference() takes and returns one part's arrays. A program takes and returns all parts, laid end to end along the dimension named above; each array names one.
All inputs are finite; a program needn't handle non-finite values.
Results may differ from the reference program's by a relative error of at most 0.001.
Values are sent between devices in bfloat16 or wider.
A program may use at most 768 MiB of HBM per device.

```python
import math
import jax
import jax.numpy as jnp
from jax import lax

NUM_ROWS = 4096
IN_DIM = 784
HIDDEN = 512
NUM_ITERS = 6
HIST_LEN = 3

IN_SCALE = 1.0 / math.sqrt(IN_DIM)
OUT_SCALE = 1.0 / math.sqrt(HIDDEN)


def setup_inputs(seed: int = 0, part: int = 0) -> dict:
    base_key = jax.random.fold_in(jax.random.key(seed), part)
    sub_keys = jax.random.split(base_key, 7)
    labels = jax.random.randint(sub_keys[0], (NUM_ROWS,), 0, 2)
    label_sign = (2 * labels - 1).astype(jnp.float32)
    mean_dir = 0.5 * jax.random.normal(sub_keys[1], (IN_DIM,), jnp.float32)
    noise_mat = jax.random.normal(sub_keys[2], (NUM_ROWS, IN_DIM), jnp.float32)
    x_data = (noise_mat + label_sign[:, None] * mean_dir[None, :]).astype(jnp.bfloat16)
    unit_pos = jnp.arange(HIDDEN, dtype=jnp.float32) / HIDDEN
    row_scale = jnp.exp2(2.0 * unit_pos - 1.0)
    w_in = jax.random.normal(sub_keys[3], (HIDDEN, IN_DIM), jnp.float32) * row_scale[:, None]
    w_out = jax.random.normal(sub_keys[4], (HIDDEN,), jnp.float32)
    reg_weight = jax.random.uniform(sub_keys[5], (1,), jnp.float32, 0.01, 0.02)
    step_size = jax.random.uniform(sub_keys[6], (1,), jnp.float32, 0.08, 0.2)
    return {"x_data": x_data, "targets": labels.astype(jnp.float32), "w_in": w_in, "w_out": w_out, "reg_weight": reg_weight, "step_size": step_size}


def fit_loss(w_in, w_out, x_f32, targets):
    pre_act = lax.dot_general(x_f32, w_in, (((1,), (1,)), ((), ()))) * IN_SCALE
    logits = jnp.dot(jnp.tanh(pre_act), w_out) * OUT_SCALE
    return jnp.mean(jax.nn.softplus(logits) - targets * logits)


def pair_dot(first, second):
    return jnp.sum(first[0] * second[0]) + jnp.sum(first[1] * second[1])


def pair_axpy(base, coef, other):
    return (base[0] + coef * other[0], base[1] + coef * other[1])


def two_loop(full_grad, hist_s, hist_y, rho_vals, gamma_scale, dot_fn):
    query_vec = full_grad
    a_coefs = {}
    for pos_idx in reversed(range(len(hist_s))):
        a_coefs[pos_idx] = rho_vals[pos_idx] * dot_fn(hist_s[pos_idx], query_vec)
        query_vec = pair_axpy(query_vec, -a_coefs[pos_idx], hist_y[pos_idx])
    result = (gamma_scale * query_vec[0], gamma_scale * query_vec[1])
    for pos_idx in range(len(hist_s)):
        b_coef = rho_vals[pos_idx] * dot_fn(hist_y[pos_idx], result)
        result = pair_axpy(result, a_coefs[pos_idx] - b_coef, hist_s[pos_idx])
    return result


def reference(x_data, targets, w_in, w_out, reg_weight, step_size):
    x_f32 = x_data.astype(jnp.float32)
    reg_coef = reg_weight[0]
    step_coef = step_size[0]
    loss_grad = jax.value_and_grad(fit_loss, argnums=(0, 1))
    params = (w_in, w_out)
    prev_params = params
    prev_grad = params
    hist_s = []
    hist_y = []
    rho_vals = []
    losses = []
    for iter_idx in range(NUM_ITERS):
        loss_val, fit_grad = loss_grad(params[0], params[1], x_f32, targets)
        losses.append(loss_val)
        full_grad = pair_axpy(fit_grad, reg_coef, params)
        if iter_idx == 0:
            direction = full_grad
        else:
            s_vec = pair_axpy(params, -1.0, prev_params)
            y_vec = pair_axpy(full_grad, -1.0, prev_grad)
            curv_ys = pair_dot(y_vec, s_vec)
            hist_s = (hist_s + [s_vec])[-HIST_LEN:]
            hist_y = (hist_y + [y_vec])[-HIST_LEN:]
            rho_vals = (rho_vals + [1.0 / curv_ys])[-HIST_LEN:]
            gamma_scale = curv_ys / pair_dot(y_vec, y_vec)
            direction = two_loop(full_grad, hist_s, hist_y, rho_vals, gamma_scale, pair_dot)
        prev_params = params
        prev_grad = full_grad
        params = pair_axpy(params, -step_coef, direction)
    return params[0], params[1], jnp.stack(losses)
```

```python
import functools
import math

import jax
import jax.numpy as jnp
from jax import lax
from jax.experimental import pallas as pl
from jax.experimental.pallas import tpu as pltpu
from jax.sharding import PartitionSpec as P

NUM_ITERS = 6
HIST = 3
CHUNKS = 4
LANES = 128
F32 = jnp.float32
BF16 = jnp.bfloat16
MESH = pl.DeviceIdType.MESH


def split3(v):
    hi = v.astype(BF16)
    rest = v - hi.astype(F32)
    mid = rest.astype(BF16)
    lo = (rest - mid.astype(F32)).astype(BF16)
    return hi, mid, lo


def kernel(
    n, rows, hid, dim, out_units,
    x_hbm, t_ref, w_ref, wo_ref, reg_ref, step_ref,
    wnew_ref, wonew_ref, loss_ref,
    xv, xt, q_ref, h_ref, u_ref, d3_ref, g3_ref, acc_ref, theta, g_ref, s_ref, y_ref, w2b_ref,
    zbuf, r_ref, dbuf, row_ref, lacc,
    xsem, zsend, zrecv, dsend, drecv,
):
    main = dim // LANES * LANES
    tail = dim - main
    width = main + LANES
    tiles = width // LANES
    groups = hid // 8
    per = rows // CHUNKS
    blocks = per // LANES
    in_scale = 1.0 / math.sqrt(dim)
    out_scale = 1.0 / math.sqrt(out_units)
    me = lax.axis_index("feat")
    reg = reg_ref[0]
    step = step_ref[0]

    def peer(d):
        return lax.rem(me + d, n)

    order = sorted(range(1, n), key=lambda d: -min(d, n - d))

    copies = [
        pltpu.make_async_copy(x_hbm.at[pl.ds(c * per, per)], xv.at[pl.ds(c * per, per)], xsem.at[c])
        for c in range(CHUNKS)
    ]
    for copy in copies:
        copy.start()
    barrier = pltpu.get_barrier_semaphore()
    for d in order:
        pl.semaphore_signal(barrier, inc=1, device_id={"feat": peer(d)}, device_id_type=MESH)

    lane8 = lax.broadcasted_iota(jnp.int32, (8, LANES), 1)
    lane = lax.broadcasted_iota(jnp.int32, (hid, LANES), 1)
    sub = lax.broadcasted_iota(jnp.int32, (hid, LANES), 0)

    def g8(v):
        return v.reshape(groups, 8, LANES)

    def col(t):
        return pl.ds(t * LANES, LANES)

    w2row = wo_ref[...]
    w2col = jnp.sum(jnp.where(lane[:, :hid] == sub[:, :hid], w2row, 0.0), axis=1, keepdims=True)
    theta[:, main:width] = jnp.where(lane == tail, w2col, 0.0)
    theta[:, 0:main] = w_ref[:, 0:main]
    theta[:, main:dim] = w_ref[:, main:dim]
    w2b_ref[...] = jnp.broadcast_to(w2col, (hid, LANES))
    s_ref[...] = jnp.zeros_like(s_ref)
    y_ref[...] = jnp.zeros_like(y_ref)
    for j in range(1, NUM_ITERS):
        q_ref[j] = jnp.zeros((hid, rows), F32)

    def pieces(src):
        for t in range(tiles):
            v = src[:, col(t)]
            if t == tiles - 1:
                v = jnp.where(lane < tail, v, 0.0)
            for i, piece in enumerate(split3(v)):
                g3_ref[i * hid:(i + 1) * hid, col(t)] = piece

    def forward(slot, c):
        rs = pl.ds(c * per, per)
        prod = lax.dot_general(g3_ref[:, 0:main], xv[rs, 0:main], (((1,), (1,)), ((), ())), preferred_element_type=F32)
        prod += lax.dot_general(g3_ref[:, main:width], xt[rs, :], (((1,), (1,)), ((), ())), preferred_element_type=F32)
        q_ref[slot, :, rs] = prod[0:hid] + (prod[hid:2 * hid] + prod[2 * hid:3 * hid])

    pieces(theta)
    for c in range(CHUNKS):
        rs = pl.ds(c * per, per)
        copies[c].wait()
        xt[rs, :] = jnp.zeros((per, LANES), BF16)
        xt[rs, 0:tail] = xv[rs, main:dim]
        forward(0, c)

    def zcopy(par, c, d):
        return pltpu.make_async_remote_copy(
            src_ref=zbuf.at[par, c, me], dst_ref=zbuf.at[par, c, me],
            send_sem=zsend.at[c, d], recv_sem=zrecv.at[par, c, me],
            device_id={"feat": peer(d)}, device_id_type=MESH)

    def zarrive(par, c, d):
        source = peer(n - d)
        return pltpu.make_async_remote_copy(
            src_ref=zbuf.at[par, c, source], dst_ref=zbuf.at[par, c, source],
            send_sem=zsend.at[c, d], recv_sem=zrecv.at[par, c, source],
            device_id={"feat": source}, device_id_type=MESH)

    def dcopy(d):
        return pltpu.make_async_remote_copy(
            src_ref=dbuf.at[me], dst_ref=dbuf.at[me], send_sem=dsend.at[d], recv_sem=drecv.at[me],
            device_id={"feat": peer(d)}, device_id_type=MESH)

    def darrive(d):
        source = peer(n - d)
        return pltpu.make_async_remote_copy(
            src_ref=dbuf.at[source], dst_ref=dbuf.at[source], send_sem=dsend.at[d], recv_sem=drecv.at[source],
            device_id={"feat": source}, device_id_type=MESH)

    def logits(par, coefs):
        for c in range(CHUNKS):
            for b in range(blocks):
                cs = col(c * blocks + b)
                pre = coefs[0] * g8(q_ref[0, :, cs])
                for j in range(1, len(coefs)):
                    pre += coefs[j] * g8(q_ref[j, :, cs])
                act = jnp.tanh(pre)
                h_ref[:, cs] = act.reshape(hid, LANES)
                part = jnp.sum(act * g8(w2b_ref[...]), axis=0)
                zbuf[par, c, me, b:b + 1, :] = jnp.sum(part, axis=0, keepdims=True) * out_scale
            for d in order:
                zcopy(par, c, d).start()
        for b in range(rows // LANES):
            act = h_ref[:, col(b)]
            u_ref[:, col(b)] = w2b_ref[...] * (1.0 - act * act)

    def gradient(it, par):
        loss = jnp.zeros((8, LANES), F32)
        gw2 = jnp.zeros((groups, 8, LANES), F32)
        for c in range(CHUNKS):
            for d in order:
                zarrive(par, c, d).wait_recv()
            z = zbuf[par, c, 0]
            for i in range(1, n):
                z += zbuf[par, c, i]
            t = t_ref[c * blocks:(c + 1) * blocks, :]
            loss += jnp.maximum(z, 0.0) + jnp.log1p(jnp.exp(-jnp.abs(z))) - t * z
            r_ref[c * blocks:(c + 1) * blocks, :] = jax.nn.sigmoid(z) - t
            for b in range(blocks):
                i = c * blocks + b
                rrow = r_ref[i:i + 1, :]
                gw2 += g8(h_ref[:, col(i)] * rrow)
                for p, piece in enumerate(split3(u_ref[:, col(i)] * rrow)):
                    d3_ref[p * hid:(p + 1) * hid, col(i)] = piece
            rs = pl.ds(c * per, per)
            lhs = d3_ref[:, rs]
            pm = jnp.dot(lhs, xv[rs, 0:main], preferred_element_type=F32)
            pt = jnp.dot(lhs, xt[rs, :], preferred_element_type=F32)
            if c == 0:
                acc_ref[:, 0:main] = pm
                acc_ref[:, main:width] = pt
            else:
                acc_ref[:, 0:main] += pm
                acc_ref[:, main:width] += pt
        lacc[it] = loss
        gw2 = jnp.sum(gw2.reshape(hid, LANES), axis=1, keepdims=True)
        for t in range(tiles):
            total = acc_ref[0:hid, col(t)] + (acc_ref[hid:2 * hid, col(t)] + acc_ref[2 * hid:3 * hid, col(t)])
            total = total * (in_scale * out_scale / rows)
            if t == tiles - 1:
                total = jnp.where(lane == tail, gw2 * (out_scale / rows), total)
            g_ref[:, col(t)] = total + reg * theta[:, col(t)]
        for c in range(CHUNKS):
            for d in order:
                zcopy(par, c, d).wait_send()

    def coefs_of(e, count):
        e = e * in_scale
        return [jnp.broadcast_to(e[:, j:j + 1], (8, LANES)) for j in range(count)]

    def broadcast(v):
        return jnp.broadcast_to(v, (8, LANES))

    pl.semaphore_wait(barrier, n - 1)
    zero = jnp.zeros((8, LANES), F32)

    logits(0, coefs_of(jnp.where(lane8 == 0, 1.0, zero), 1))
    gradient(0, 0)
    pieces(g_ref)
    for c in range(CHUNKS):
        forward(1, c)
    for t in range(tiles):
        s = -step * g_ref[:, col(t)]
        s_ref[0, :, col(t)] = s
        theta[:, col(t)] += s
    sig = jnp.where(lane8 == 1, -step, zero)
    e = jnp.where(lane8 == 0, 1.0, sig)

    for i in range(6):
        row_ref[i] = zero
    for i, v in enumerate((sig, zero, zero, e)):
        row_ref[6 + i] = v

    def body(k, carry):
        rho1, rho2, sy21, yy11, yy12, yy22, sig0, sig1, sig2, e = (row_ref[i] for i in range(10))
        par = lax.rem(k, 2)
        slots = [lax.rem(k + 2 - a, HIST) for a in range(HIST)]
        last = width - LANES
        w2b_ref[...] = jnp.broadcast_to(theta[:, last + tail:last + tail + 1], (hid, LANES))
        logits(par, coefs_of(e, NUM_ITERS))
        for t in range(tiles):
            y_ref[slots[0], :, col(t)] = g_ref[:, col(t)]
        gradient(k, par)
        dots = [jnp.zeros((8, LANES), F32)] * 12
        for t in range(tiles):
            g = g8(g_ref[:, col(t)])
            y0 = g - g8(y_ref[slots[0], :, col(t)])
            y_ref[slots[0], :, col(t)] = y0.reshape(hid, LANES)
            ss = [g8(s_ref[slots[a], :, col(t)]) for a in range(HIST)]
            ys = [y0] + [g8(y_ref[slots[a], :, col(t)]) for a in range(1, HIST)]
            pairs = [(v, g) for v in ss] + [(v, g) for v in ys] + [(v, y0) for v in ss] + [(v, y0) for v in ys]
            dots = [d + jnp.sum(a * b, axis=0) for d, (a, b) in zip(dots, pairs)]
        row = jnp.zeros((1, LANES), F32)
        for i, d in enumerate(dots):
            d = jnp.sum(jnp.sum(d, axis=0, keepdims=True), axis=1, keepdims=True)
            row = jnp.where(lane8[0:1] == i, d, row)
        dbuf[me] = row
        for d in order:
            dcopy(d).start()

        @pl.when(k < NUM_ITERS - 1)
        def _():
            pieces(g_ref)
            for c in range(CHUNKS):
                forward(k + 1, c)

        for d in order:
            darrive(d).wait_recv()
        total = dbuf[0]
        for i in range(1, n):
            total += dbuf[i]
        vals = [broadcast(total[:, i:i + 1]) for i in range(12)]
        sg, yg, y0s, y0y = vals[0:3], vals[3:6], vals[6:9], vals[9:12]
        rho = [1.0 / y0s[0], rho1, rho2]
        gamma = y0s[0] / y0y[0]
        sy = {(1, 0): y0s[1], (2, 0): y0s[2], (2, 1): sy21}
        yy = {(0, 0): y0y[0], (0, 1): y0y[1], (0, 2): y0y[2], (1, 1): yy11, (1, 2): yy12, (2, 2): yy22}
        a = []
        for i in range(HIST):
            v = sg[i]
            for j in range(i):
                v = v - a[j] * sy[i, j]
            a.append(rho[i] * v)
        diff = [None] * HIST
        for i in reversed(range(HIST)):
            v = yg[i]
            for j in range(HIST):
                v = v - a[j] * yy[min(i, j), max(i, j)]
            v = gamma * v
            for j in range(i + 1, HIST):
                v = v + diff[j] * sy[j, i]
            diff[i] = a[i] - rho[i] * v
        cg = -step * gamma
        cy = [-cg * v for v in a]
        cs = [-step * v for v in diff]
        sigs = [sig0, sig1, sig2]
        new = jnp.where(lane8 == k + 1, cg, zero)
        for i in range(HIST):
            new = new + jnp.where(lane8 == k + 1 - i, cy[i], zero) - jnp.where(lane8 == k - i, cy[i], zero)
            new = new + cs[i] * sigs[i]
        for t in range(tiles):
            s = cg * g8(g_ref[:, col(t)])
            for i in range(HIST):
                s = s + cy[i] * g8(y_ref[slots[i], :, col(t)])
                s = s + cs[i] * g8(s_ref[slots[i], :, col(t)])
            s = s.reshape(hid, LANES)
            s_ref[slots[2], :, col(t)] = s
            theta[:, col(t)] += s
        for d in order:
            dcopy(d).wait_send()
        for i, v in enumerate((rho[0], rho[1], sy[1, 0], yy[0, 0], yy[0, 1], yy[1, 1], new, sig0, sig1, e + new)):
            row_ref[i] = v
        return carry

    lax.fori_loop(1, NUM_ITERS, body, 0)

    wnew_ref[:, 0:main] = theta[:, 0:main]
    wnew_ref[:, main:dim] = theta[:, main:dim]
    w2col = theta[:, dim:dim + 1]
    wonew_ref[...] = jnp.sum(jnp.where(lane == sub, w2col, 0.0), axis=0, keepdims=True)[:, 0:hid]
    for k in range(NUM_ITERS):
        loss_ref[k] = jnp.sum(lacc[k]) / rows


def solution(mesh):
    n = mesh.shape["feat"]

    def local_solve(x, t, w, wo, reg, step):
        rows, dim = x.shape
        hid = w.shape[0]
        width = dim // LANES * LANES + LANES
        per = rows // CHUNKS
        vmem = pl.BlockSpec(memory_space=pltpu.VMEM)
        smem = pl.BlockSpec(memory_space=pltpu.SMEM)
        wnew, wonew, losses = pl.pallas_call(
            functools.partial(kernel, n, rows, hid, dim, hid * n),
            out_shape=(
                jax.ShapeDtypeStruct((hid, dim), F32),
                jax.ShapeDtypeStruct((1, hid), F32),
                jax.ShapeDtypeStruct((NUM_ITERS,), F32),
            ),
            in_specs=[pl.BlockSpec(memory_space=pltpu.HBM), vmem, vmem, vmem, smem, smem],
            out_specs=(vmem, vmem, smem),
            scratch_shapes=[
                pltpu.VMEM((rows, dim), BF16),
                pltpu.VMEM((rows, LANES), BF16),
                pltpu.VMEM((NUM_ITERS, hid, rows), F32),
                pltpu.VMEM((hid, rows), F32),
                pltpu.VMEM((hid, rows), F32),
                pltpu.VMEM((3 * hid, rows), BF16),
                pltpu.VMEM((3 * hid, width), BF16),
                pltpu.VMEM((3 * hid, width), F32),
                pltpu.VMEM((hid, width), F32),
                pltpu.VMEM((hid, width), F32),
                pltpu.VMEM((HIST, hid, width), F32),
                pltpu.VMEM((HIST, hid, width), F32),
                pltpu.VMEM((hid, LANES), F32),
                pltpu.VMEM((2, CHUNKS, n, per // LANES, LANES), F32),
                pltpu.VMEM((rows // LANES, LANES), F32),
                pltpu.VMEM((n, 1, LANES), F32),
                pltpu.VMEM((10, 8, LANES), F32),
                pltpu.VMEM((NUM_ITERS, 8, LANES), F32),
                pltpu.SemaphoreType.DMA((CHUNKS,)),
                pltpu.SemaphoreType.DMA((CHUNKS, n)),
                pltpu.SemaphoreType.DMA((2, CHUNKS, n)),
                pltpu.SemaphoreType.DMA((n,)),
                pltpu.SemaphoreType.DMA((n,)),
            ],
            compiler_params=pltpu.CompilerParams(
                collective_id=0, has_side_effects=True, vmem_limit_bytes=56 * 1024 * 1024
            ),
        )(x, t.reshape(rows // LANES, LANES), w, wo.reshape(1, hid), reg, step)
        return wnew, wonew.reshape(hid), losses

    specs_in = (P("prob", None), P("prob"), P(("prob", "feat"), None), P(("prob", "feat")), P("prob"), P("prob"))
    specs_out = (P(("prob", "feat"), None), P(("prob", "feat")), P("prob"))
    return jax.shard_map(local_solve, mesh=mesh, in_specs=specs_in, out_specs=specs_out, check_vma=False)
```

```python
import functools
import math

import jax
import jax.numpy as jnp
from jax import lax
from jax.experimental import pallas as pl
from jax.experimental.pallas import tpu as pltpu
from jax.sharding import PartitionSpec as P

NUM_ITERS = 6
HIST = 3
CHUNKS = 4
LANES = 128
F32 = jnp.float32
BF16 = jnp.bfloat16
MESH = pl.DeviceIdType.MESH


def split3(v):
    hi = v.astype(BF16)
    rest = v - hi.astype(F32)
    mid = rest.astype(BF16)
    lo = (rest - mid.astype(F32)).astype(BF16)
    return hi, mid, lo


def kernel(
    n, rows, hid, dim, out_units,
    x_hbm, t_hbm, w_hbm, wo_hbm, reg_hbm, step_hbm,
    theta, lacc,
    xv, xr, xt, t_ref, w_ref, wo_ref, reg_ref, step_ref, q_ref, h_ref, u_ref, d3_ref, g3_ref, gt_ref, acc_ref, g_ref, s_ref, y_ref, w2b_ref,
    zbuf, r_ref, dbuf, row_ref,
    xsem, isem, zsend, zrecv, dsend, drecv,
):
    main = dim // LANES * LANES
    tail = dim - main
    width = main + LANES
    tiles = width // LANES
    groups = hid // 8
    per = rows // CHUNKS
    blocks = per // LANES
    in_scale = 1.0 / math.sqrt(dim)
    out_scale = 1.0 / math.sqrt(out_units)
    me = lax.axis_index("feat")

    def peer(d):
        return lax.rem(me + d, n)

    order = sorted(range(1, n), key=lambda d: -min(d, n - d))

    copies = [
        pltpu.make_async_copy(x_hbm.at[:, pl.ds(c * per, per)], xr.at[:, pl.ds(c * per, per)], xsem.at[c])
        for c in range(CHUNKS)
    ]
    inputs = [
        pltpu.make_async_copy(src, dst, isem.at[i])
        for i, (src, dst) in enumerate(
            ((w_hbm, w_ref), (wo_hbm, wo_ref), (t_hbm, t_ref), (reg_hbm, reg_ref), (step_hbm, step_ref)))
    ]
    for copy in inputs[:2] + copies + inputs[2:]:
        copy.start()
    barrier = pltpu.get_barrier_semaphore()
    for d in order:
        pl.semaphore_signal(barrier, inc=1, device_id={"feat": peer(d)}, device_id_type=MESH)

    lane8 = lax.broadcasted_iota(jnp.int32, (8, LANES), 1)
    lane = lax.broadcasted_iota(jnp.int32, (hid, LANES), 1)
    sub = lax.broadcasted_iota(jnp.int32, (hid, LANES), 0)

    def g8(v):
        return v.reshape(groups, 8, LANES)

    def col(t):
        return pl.ds(t * LANES, LANES)

    for copy in inputs:
        copy.wait()
    reg = reg_ref[0]
    step = step_ref[0]

    w2row = wo_ref[...]
    w2col = jnp.sum(jnp.where(lane[:, :hid] == sub[:, :hid], w2row, 0.0), axis=1, keepdims=True)
    theta[:, main:width] = jnp.where(lane == tail, w2col, 0.0)
    theta[:, 0:main] = w_ref[:, 0:main]
    theta[:, main:dim] = w_ref[:, main:dim]
    w2b_ref[...] = jnp.broadcast_to(w2col, (hid, LANES))
    s_ref[...] = jnp.zeros_like(s_ref)
    y_ref[...] = jnp.zeros_like(y_ref)
    for j in range(1, NUM_ITERS):
        q_ref[j] = jnp.zeros((hid, rows), F32)

    def pieces(src):
        for t in range(tiles - 1):
            for i, piece in enumerate(split3(src[:, col(t)])):
                g3_ref[i * hid:(i + 1) * hid, col(t)] = piece
        for i, piece in enumerate(split3(src[:, main:dim])):
            gt_ref[:, i * tail:(i + 1) * tail] = piece

    def forward(slot, c):
        rs = pl.ds(c * per, per)
        prod = jnp.dot(g3_ref[...], xr[0:main, rs], preferred_element_type=F32)
        prod_t = jnp.dot(gt_ref[...], xt[:, rs], preferred_element_type=F32)
        q_ref[slot, :, rs] = prod[0:hid] + (prod[hid:2 * hid] + (prod[2 * hid:3 * hid] + prod_t))

    gt_ref[...] = jnp.zeros_like(gt_ref)
    xt[3 * tail:, :] = jnp.zeros((LANES - 3 * tail, rows), BF16)
    pieces(theta)
    for c in range(CHUNKS):
        rs = pl.ds(c * per, per)
        copies[c].wait()
        for i in range(3):
            xt[i * tail:(i + 1) * tail, rs] = xr[main:dim, rs]
        forward(0, c)

    def by_rows():
        for c in range(rows // LANES):
            for t in range(tiles - 1):
                xv[col(c), col(t)] = xr[col(t), col(c)].T
            xv[col(c), main:width] = xt[:, col(c)].T

    def zcopy(par, c, d):
        return pltpu.make_async_remote_copy(
            src_ref=zbuf.at[par, c, me], dst_ref=zbuf.at[par, c, me],
            send_sem=zsend.at[c, d], recv_sem=zrecv.at[par, c, me],
            device_id={"feat": peer(d)}, device_id_type=MESH)

    def zarrive(par, c, d):
        source = peer(n - d)
        return pltpu.make_async_remote_copy(
            src_ref=zbuf.at[par, c, source], dst_ref=zbuf.at[par, c, source],
            send_sem=zsend.at[c, d], recv_sem=zrecv.at[par, c, source],
            device_id={"feat": source}, device_id_type=MESH)

    def dcopy(d):
        return pltpu.make_async_remote_copy(
            src_ref=dbuf.at[me], dst_ref=dbuf.at[me], send_sem=dsend.at[d], recv_sem=drecv.at[me],
            device_id={"feat": peer(d)}, device_id_type=MESH)

    def darrive(d):
        source = peer(n - d)
        return pltpu.make_async_remote_copy(
            src_ref=dbuf.at[source], dst_ref=dbuf.at[source], send_sem=dsend.at[d], recv_sem=drecv.at[source],
            device_id={"feat": source}, device_id_type=MESH)

    def logits(par, coefs):
        for c in range(CHUNKS):
            for b in range(blocks):
                cs = col(c * blocks + b)
                pre = coefs[0] * g8(q_ref[0, :, cs])
                for j in range(1, len(coefs)):
                    pre += coefs[j] * g8(q_ref[j, :, cs])
                act = jnp.tanh(pre)
                h_ref[:, cs] = act.reshape(hid, LANES)
                part = jnp.sum(act * g8(w2b_ref[...]), axis=0)
                zbuf[par, c, me, b:b + 1, :] = jnp.sum(part, axis=0, keepdims=True) * out_scale
            for d in order:
                zcopy(par, c, d).start()
        for b in range(rows // LANES):
            act = h_ref[:, col(b)]
            u_ref[:, col(b)] = w2b_ref[...] * (1.0 - act * act)

    def gradient(it, par):
        loss = jnp.zeros((8, LANES), F32)
        gw2 = jnp.zeros((groups, 8, LANES), F32)
        for c in range(CHUNKS):
            for d in order:
                zarrive(par, c, d).wait_recv()
            z = zbuf[par, c, 0]
            for i in range(1, n):
                z += zbuf[par, c, i]
            t = t_ref[c * blocks:(c + 1) * blocks, :]
            loss += jnp.maximum(z, 0.0) + jnp.log1p(jnp.exp(-jnp.abs(z))) - t * z
            r_ref[c * blocks:(c + 1) * blocks, :] = jax.nn.sigmoid(z) - t
            for b in range(blocks):
                i = c * blocks + b
                rrow = r_ref[i:i + 1, :]
                gw2 += g8(h_ref[:, col(i)] * rrow)
                for p, piece in enumerate(split3(u_ref[:, col(i)] * rrow)):
                    d3_ref[p * hid:(p + 1) * hid, col(i)] = piece
            rs = pl.ds(c * per, per)
            lhs = d3_ref[:, rs]
            prod = jnp.dot(lhs, xv[rs, :], preferred_element_type=F32)
            if c == 0:
                acc_ref[...] = prod
            else:
                acc_ref[...] += prod
        lacc[it] = loss
        gw2 = jnp.sum(gw2.reshape(hid, LANES), axis=1, keepdims=True)
        for t in range(tiles):
            total = acc_ref[0:hid, col(t)] + (acc_ref[hid:2 * hid, col(t)] + acc_ref[2 * hid:3 * hid, col(t)])
            total = total * (in_scale * out_scale / rows)
            if t == tiles - 1:
                total = jnp.where(lane < tail, total, jnp.where(lane == tail, gw2 * (out_scale / rows), 0.0))
            g_ref[:, col(t)] = total + reg * theta[:, col(t)]
        for c in range(CHUNKS):
            for d in order:
                zcopy(par, c, d).wait_send()

    def coefs_of(e, count):
        e = e * in_scale
        return [jnp.broadcast_to(e[:, j:j + 1], (8, LANES)) for j in range(count)]

    def broadcast(v):
        return jnp.broadcast_to(v, (8, LANES))

    pl.semaphore_wait(barrier, n - 1)
    zero = jnp.zeros((8, LANES), F32)

    logits(0, coefs_of(jnp.where(lane8 == 0, 1.0, zero), 1))
    by_rows()
    gradient(0, 0)
    pieces(g_ref)
    for c in range(CHUNKS):
        forward(1, c)
    for t in range(tiles):
        s = -step * g_ref[:, col(t)]
        s_ref[0, :, col(t)] = s
        theta[:, col(t)] += s
    sig = jnp.where(lane8 == 1, -step, zero)
    e = jnp.where(lane8 == 0, 1.0, sig)

    for i in range(6):
        row_ref[i] = zero
    for i, v in enumerate((sig, zero, zero, e)):
        row_ref[6 + i] = v

    def body(k, carry):
        rho1, rho2, sy21, yy11, yy12, yy22, sig0, sig1, sig2, e = (row_ref[i] for i in range(10))
        par = lax.rem(k, 2)
        slots = [lax.rem(k + 2 - a, HIST) for a in range(HIST)]
        last = width - LANES
        w2b_ref[...] = jnp.broadcast_to(theta[:, last + tail:last + tail + 1], (hid, LANES))
        logits(par, coefs_of(e, NUM_ITERS))
        for t in range(tiles):
            y_ref[slots[0], :, col(t)] = g_ref[:, col(t)]
        gradient(k, par)
        dots = [jnp.zeros((8, LANES), F32)] * 12
        for t in range(tiles):
            g = g8(g_ref[:, col(t)])
            y0 = g - g8(y_ref[slots[0], :, col(t)])
            y_ref[slots[0], :, col(t)] = y0.reshape(hid, LANES)
            ss = [g8(s_ref[slots[a], :, col(t)]) for a in range(HIST)]
            ys = [y0] + [g8(y_ref[slots[a], :, col(t)]) for a in range(1, HIST)]
            pairs = [(v, g) for v in ss] + [(v, g) for v in ys] + [(v, y0) for v in ss] + [(v, y0) for v in ys]
            dots = [d + jnp.sum(a * b, axis=0) for d, (a, b) in zip(dots, pairs)]
        row = jnp.zeros((1, LANES), F32)
        for i, d in enumerate(dots):
            d = jnp.sum(jnp.sum(d, axis=0, keepdims=True), axis=1, keepdims=True)
            row = jnp.where(lane8[0:1] == i, d, row)
        dbuf[me] = row
        for d in order:
            dcopy(d).start()

        @pl.when(k < NUM_ITERS - 1)
        def _():
            pieces(g_ref)
            for c in range(CHUNKS):
                forward(k + 1, c)

        for d in order:
            darrive(d).wait_recv()
        total = dbuf[0]
        for i in range(1, n):
            total += dbuf[i]
        vals = [broadcast(total[:, i:i + 1]) for i in range(12)]
        sg, yg, y0s, y0y = vals[0:3], vals[3:6], vals[6:9], vals[9:12]
        rho = [1.0 / y0s[0], rho1, rho2]
        gamma = y0s[0] / y0y[0]
        sy = {(1, 0): y0s[1], (2, 0): y0s[2], (2, 1): sy21}
        yy = {(0, 0): y0y[0], (0, 1): y0y[1], (0, 2): y0y[2], (1, 1): yy11, (1, 2): yy12, (2, 2): yy22}
        a = []
        for i in range(HIST):
            v = sg[i]
            for j in range(i):
                v = v - a[j] * sy[i, j]
            a.append(rho[i] * v)
        diff = [None] * HIST
        for i in reversed(range(HIST)):
            v = yg[i]
            for j in range(HIST):
                v = v - a[j] * yy[min(i, j), max(i, j)]
            v = gamma * v
            for j in range(i + 1, HIST):
                v = v + diff[j] * sy[j, i]
            diff[i] = a[i] - rho[i] * v
        cg = -step * gamma
        cy = [-cg * v for v in a]
        cs = [-step * v for v in diff]
        sigs = [sig0, sig1, sig2]
        new = jnp.where(lane8 == k + 1, cg, zero)
        for i in range(HIST):
            new = new + jnp.where(lane8 == k + 1 - i, cy[i], zero) - jnp.where(lane8 == k - i, cy[i], zero)
            new = new + cs[i] * sigs[i]
        for t in range(tiles):
            s = cg * g8(g_ref[:, col(t)])
            for i in range(HIST):
                s = s + cy[i] * g8(y_ref[slots[i], :, col(t)])
                s = s + cs[i] * g8(s_ref[slots[i], :, col(t)])
            s = s.reshape(hid, LANES)
            s_ref[slots[2], :, col(t)] = s
            theta[:, col(t)] += s
        for d in order:
            dcopy(d).wait_send()
        for i, v in enumerate((rho[0], rho[1], sy[1, 0], yy[0, 0], yy[0, 1], yy[1, 1], new, sig0, sig1, e + new)):
            row_ref[i] = v
        return carry

    lax.fori_loop(1, NUM_ITERS, body, 0)


def unpack(rows, theta, lacc, wnew_ref, wonew_ref, loss_ref):
    hid, dim = wnew_ref.shape
    wnew_ref[...] = theta[:, 0:dim]
    lane = lax.broadcasted_iota(jnp.int32, (hid, LANES), 1)
    sub = lax.broadcasted_iota(jnp.int32, (hid, LANES), 0)
    w2col = theta[:, dim:dim + 1]
    wonew_ref[...] = jnp.sum(jnp.where(lane == sub, w2col, 0.0), axis=0, keepdims=True)[:, 0:hid]
    row = jnp.zeros((1, LANES), F32)
    for k in range(NUM_ITERS):
        loss = jnp.sum(jnp.sum(lacc[k], axis=0, keepdims=True), axis=1, keepdims=True)
        row = jnp.where(lane[0:1] == k, loss, row)
    loss_ref[...] = row[:, 0:NUM_ITERS] / rows


def solution(mesh):
    n = mesh.shape["feat"]

    def local_solve(x, t, w, wo, reg, step):
        rows, dim = x.shape
        hid = w.shape[0]
        width = dim // LANES * LANES + LANES
        per = rows // CHUNKS
        vmem = pl.BlockSpec(memory_space=pltpu.VMEM)
        hbm = pl.BlockSpec(memory_space=pltpu.HBM)
        theta, lacc = pl.pallas_call(
            functools.partial(kernel, n, rows, hid, dim, hid * n),
            out_shape=(
                jax.ShapeDtypeStruct((hid, width), F32),
                jax.ShapeDtypeStruct((NUM_ITERS, 8, LANES), F32),
            ),
            in_specs=[hbm] * 6,
            out_specs=(vmem, vmem),
            scratch_shapes=[
                pltpu.VMEM((rows, width), BF16),
                pltpu.VMEM((dim, rows), BF16),
                pltpu.VMEM((LANES, rows), BF16),
                pltpu.VMEM((rows // LANES, LANES), F32),
                pltpu.VMEM((hid, dim), F32),
                pltpu.VMEM((1, hid), F32),
                pltpu.SMEM((1,), F32),
                pltpu.SMEM((1,), F32),
                pltpu.VMEM((NUM_ITERS, hid, rows), F32),
                pltpu.VMEM((hid, rows), F32),
                pltpu.VMEM((hid, rows), F32),
                pltpu.VMEM((3 * hid, rows), BF16),
                pltpu.VMEM((3 * hid, dim // LANES * LANES), BF16),
                pltpu.VMEM((hid, LANES), BF16),
                pltpu.VMEM((3 * hid, width), F32),
                pltpu.VMEM((hid, width), F32),
                pltpu.VMEM((HIST, hid, width), F32),
                pltpu.VMEM((HIST, hid, width), F32),
                pltpu.VMEM((hid, LANES), F32),
                pltpu.VMEM((2, CHUNKS, n, per // LANES, LANES), F32),
                pltpu.VMEM((rows // LANES, LANES), F32),
                pltpu.VMEM((n, 1, LANES), F32),
                pltpu.VMEM((10, 8, LANES), F32),
                pltpu.SemaphoreType.DMA((CHUNKS,)),
                pltpu.SemaphoreType.DMA((5,)),
                pltpu.SemaphoreType.DMA((CHUNKS, n)),
                pltpu.SemaphoreType.DMA((2, CHUNKS, n)),
                pltpu.SemaphoreType.DMA((n,)),
                pltpu.SemaphoreType.DMA((n,)),
            ],
            compiler_params=pltpu.CompilerParams(
                collective_id=0, has_side_effects=True, vmem_limit_bytes=56 * 1024 * 1024
            ),
        )(x.T, t.reshape(rows // LANES, LANES), w, wo.reshape(1, hid), reg, step)
        wnew, wonew, losses = pl.pallas_call(
            functools.partial(unpack, rows),
            out_shape=(
                jax.ShapeDtypeStruct((hid, dim), F32),
                jax.ShapeDtypeStruct((1, hid), F32),
                jax.ShapeDtypeStruct((1, NUM_ITERS), F32),
            ),
            in_specs=[vmem, vmem],
            out_specs=(vmem,) * 3,
        )(theta, lacc)
        return wnew, wonew.reshape(hid), losses.reshape(NUM_ITERS)

    specs_in = (P("prob", None), P("prob"), P(("prob", "feat"), None), P(("prob", "feat")), P("prob"), P("prob"))
    specs_out = (P(("prob", "feat"), None), P(("prob", "feat")), P("prob"))
    return jax.shard_map(local_solve, mesh=mesh, in_specs=specs_in, out_specs=specs_out, check_vma=False)
```

```python
import functools
import math

import jax
import jax.numpy as jnp
from jax import lax
from jax.experimental import pallas as pl
from jax.experimental.pallas import tpu as pltpu
from jax.sharding import PartitionSpec as P

NUM_ITERS = 6
HIST = 3
CHUNKS = 4
SPLIT = (1, 1, 2)
VMEM_BYTES = 50 * 1024 * 1024
LANES = 128
F32 = jnp.float32
BF16 = jnp.bfloat16
MESH = pl.DeviceIdType.MESH


def split3(v):
    hi = v.astype(BF16)
    rest = v - hi.astype(F32)
    mid = rest.astype(BF16)
    lo = (rest - mid.astype(F32)).astype(BF16)
    return hi, mid, lo


def kernel(
    n, rows, hid, dim, out_units,
    x_hbm, t_hbm, w_hbm, wo_hbm, reg_ref, step_ref,
    theta, lacc,
    xv, xr, xt, t_ref, w_ref, wo_ref, q_ref, h_ref, u_ref, d3_ref, g3_ref, gt_ref, acc_ref, tail_ref, g_ref,
    s_ref, y_ref, w2b_ref, zbuf, r_ref, dbuf,
    xsem, isem, zsend, zrecv, dsend, drecv,
):
    main = dim // LANES * LANES
    tail = dim - main
    width = main + LANES
    tiles = width // LANES
    groups = hid // 8
    per = rows // CHUNKS
    blocks = per // LANES
    sizes = [v * rows // (sum(SPLIT) * LANES) for v in SPLIT]
    spans = [(sum(sizes[:i]), sum(sizes[:i + 1])) for i in range(len(sizes))]
    in_scale = 1.0 / math.sqrt(dim)
    out_scale = 1.0 / math.sqrt(out_units)
    me = lax.axis_index("feat")

    def peer(d):
        return lax.rem(me + d, n)

    order = sorted(range(1, n), key=lambda d: -min(d, n - d))

    copies = [
        pltpu.make_async_copy(x_hbm.at[:, pl.ds(c * per, per)], xr.at[:, pl.ds(c * per, per)], xsem.at[c])
        for c in range(CHUNKS)
    ]
    inputs = [
        pltpu.make_async_copy(src, dst, isem.at[i])
        for i, (src, dst) in enumerate(
            ((w_hbm, w_ref), (wo_hbm, wo_ref), (t_hbm, t_ref)))
    ]
    for copy in inputs[:2] + copies + inputs[2:]:
        copy.start()
    barrier = pltpu.get_barrier_semaphore()
    for d in order:
        pl.semaphore_signal(barrier, inc=1, device_id={"feat": peer(d)}, device_id_type=MESH)

    lane8 = lax.broadcasted_iota(jnp.int32, (8, LANES), 1)
    lane = lax.broadcasted_iota(jnp.int32, (hid, LANES), 1)
    sub = lax.broadcasted_iota(jnp.int32, (hid, LANES), 0)

    def g8(v):
        return v.reshape(groups, 8, LANES)

    def col(t):
        return pl.ds(t * LANES, LANES)

    def pieces(src):
        for t in range(tiles - 1):
            for i, piece in enumerate(split3(src[:, col(t)])):
                g3_ref[i * hid:(i + 1) * hid, col(t)] = piece
        for i, piece in enumerate(split3(src[:, main:dim])):
            gt_ref[:, i * tail:(i + 1) * tail] = piece

    def forward(slot, rs):
        prod = jnp.dot(g3_ref[...], xr[0:main, rs], preferred_element_type=F32)
        prod_t = jnp.dot(gt_ref[...], xt[:, rs], preferred_element_type=F32)
        q_ref[slot, :, rs] = prod[0:hid] + (prod[hid:2 * hid] + (prod[2 * hid:3 * hid] + prod_t))

    def zcopy(par, c, d):
        return pltpu.make_async_remote_copy(
            src_ref=zbuf.at[par, me, pl.ds(spans[c][0], sizes[c])], dst_ref=zbuf.at[par, me, pl.ds(spans[c][0], sizes[c])],
            send_sem=zsend.at[c, d], recv_sem=zrecv.at[par, c, me],
            device_id={"feat": peer(d)}, device_id_type=MESH)

    def zarrive(par, c, d):
        source = peer(n - d)
        return pltpu.make_async_remote_copy(
            src_ref=zbuf.at[par, source, pl.ds(spans[c][0], sizes[c])],
            dst_ref=zbuf.at[par, source, pl.ds(spans[c][0], sizes[c])],
            send_sem=zsend.at[c, d], recv_sem=zrecv.at[par, c, source],
            device_id={"feat": source}, device_id_type=MESH)

    def dcopy(d):
        return pltpu.make_async_remote_copy(
            src_ref=dbuf.at[me], dst_ref=dbuf.at[me], send_sem=dsend.at[d], recv_sem=drecv.at[me],
            device_id={"feat": peer(d)}, device_id_type=MESH)

    def darrive(d):
        source = peer(n - d)
        return pltpu.make_async_remote_copy(
            src_ref=dbuf.at[source], dst_ref=dbuf.at[source], send_sem=dsend.at[d], recv_sem=drecv.at[source],
            device_id={"feat": source}, device_id_type=MESH)

    def logits(par, coefs, start, stop):
        scaled = [v * in_scale for v in coefs]
        for b in range(start, stop):
            cs = col(b)
            pre = scaled[0] * g8(q_ref[0, :, cs])
            for j in range(1, len(coefs)):
                pre += scaled[j] * g8(q_ref[j, :, cs])
            act = jnp.tanh(pre)
            h_ref[:, cs] = act.reshape(hid, LANES)
            part = jnp.sum(act * g8(w2b_ref[...]), axis=0)
            zbuf[par, me, b:b + 1, :] = jnp.sum(part, axis=0, keepdims=True) * out_scale
        for c, span in enumerate(spans):
            if start < span[1] <= stop:
                for d in order:
                    zcopy(par, c, d).start()

    def slopes():
        for b in range(rows // LANES):
            act = h_ref[:, col(b)]
            u_ref[:, col(b)] = w2b_ref[...] * (1.0 - act * act)

    def gradient(it, par, reg, use):
        loss = jnp.zeros((8, LANES), F32)
        gw2 = jnp.zeros((groups, 8, LANES), F32)
        for c, (start, stop) in enumerate(spans):
            for d in order:
                zarrive(par, c, d).wait_recv()
            z = zbuf[par, 0, start:stop, :]
            for i in range(1, n):
                z += zbuf[par, i, start:stop, :]
            t = t_ref[start:stop, :]
            cost = jnp.maximum(z, 0.0) + jnp.log1p(jnp.exp(-jnp.abs(z))) - t * z
            loss += jnp.sum(cost.reshape((stop - start) // 8, 8, LANES), axis=0)
            r_ref[start:stop, :] = jax.nn.sigmoid(z) - t
            for i in range(start, stop):
                rrow = r_ref[i:i + 1, :]
                gw2 += g8(h_ref[:, col(i)] * rrow)
                for p, piece in enumerate(split3(u_ref[:, col(i)] * rrow)):
                    d3_ref[p * hid:(p + 1) * hid, col(i)] = piece
            rs = pl.ds(start * LANES, (stop - start) * LANES)
            prod_t = lax.dot_general(
                xr[main:dim, rs], d3_ref[:, rs], (((1,), (1,)), ((), ())), preferred_element_type=F32)
            last = prod_t if c == 0 else last + prod_t
            if c < len(spans) - 1:
                prod = jnp.dot(d3_ref[:, rs], xv[rs, :], preferred_element_type=F32)
                if c == 0:
                    acc_ref[...] = prod
                else:
                    acc_ref[...] += prod
        lacc[it] = loss
        gw2 = jnp.sum(gw2.reshape(hid, LANES), axis=1, keepdims=True)
        rs = pl.ds(spans[-1][0] * LANES, sizes[-1] * LANES)
        def finish(t, total):
            g_ref[par, :, col(t)] = (g8(total) + reg * g8(theta[:, col(t)])).reshape(hid, LANES)
            use(t)

        scale = in_scale * out_scale / rows
        for start in range(0, main, 2 * LANES):
            cs = slice(start, start + 2 * LANES)
            prod = jnp.dot(d3_ref[:, rs], xv[rs, cs], preferred_element_type=F32) + acc_ref[:, cs]
            prod = (prod[0:hid] + (prod[hid:2 * hid] + prod[2 * hid:3 * hid])) * scale
            finish(start // LANES, prod[:, :LANES])
            finish(start // LANES + 1, prod[:, LANES:])
            if start == 0:
                last = last[:, 0:hid] + (last[:, hid:2 * hid] + last[:, 2 * hid:3 * hid])
                tail_ref[:, 0:tail] = last.T * scale
                finish(tiles - 1, jnp.where(lane == tail, gw2 * (out_scale / rows), tail_ref[...]))

    def sent(par):
        for c in range(len(spans)):
            for d in order:
                zcopy(par, c, d).wait_send()

    def by_rows():
        def rows_of(c, carry):
            cs = pl.ds(pl.multiple_of(c * 2 * LANES, 2 * LANES), 2 * LANES)
            for t in range(tiles - 1):
                xv[cs, col(t)] = xr[col(t), cs].T
            return carry

        lax.fori_loop(0, rows // (2 * LANES), rows_of, 0)

    gt_ref[...] = jnp.zeros_like(gt_ref)
    tail_ref[...] = jnp.zeros_like(tail_ref)
    xt[3 * tail:, :] = jnp.zeros((LANES - 3 * tail, rows), BF16)
    for copy in inputs[:2]:
        copy.wait()
    w2col = jnp.sum(jnp.where(lane[:, :hid] == sub[:, :hid], wo_ref[...], 0.0), axis=1, keepdims=True)
    theta[:, main:width] = jnp.where(lane == tail, w2col, 0.0)
    theta[:, 0:main] = w_ref[:, 0:main]
    theta[:, main:dim] = w_ref[:, main:dim]
    w2b_ref[...] = jnp.broadcast_to(w2col, (hid, LANES))
    pieces(theta)
    pl.semaphore_wait(barrier, n - 1)

    one = jnp.ones((8, LANES), F32)
    for c in range(CHUNKS):
        rs = pl.ds(c * per, per)
        copies[c].wait()
        for i in range(3):
            xt[i * tail:(i + 1) * tail, rs] = xr[main:dim, rs]
        forward(0, rs)
        logits(0, [one], c * blocks, (c + 1) * blocks)
    for copy in inputs[2:]:
        copy.wait()
    reg = jnp.full((8, LANES), reg_ref[0], F32)
    step = jnp.full((8, LANES), step_ref[0], F32)
    slopes()
    by_rows()

    def first(t):
        s = -step * g8(g_ref[0, :, col(t)])
        s_ref[0, :, col(t)] = s.reshape(hid, LANES)
        theta[:, col(t)] = (g8(theta[:, col(t)]) + s).reshape(hid, LANES)

    gradient(0, 0, reg, first)
    pieces(g_ref.at[0])
    coefs = [one, -step]
    sigma = {0: [-step]}
    w2b_ref[...] = jnp.broadcast_to(theta[:, dim:dim + 1], (hid, LANES))
    for c in range(CHUNKS):
        rs = pl.ds(c * per, per)
        forward(1, rs)
        logits(1, coefs, c * blocks, (c + 1) * blocks)
    sent(0)

    rho, sy, yy, sg, yg = {}, {}, {}, {}, {}
    update = None
    for k in range(1, NUM_ITERS):
        par = k % 2
        if k > 1:
            w2b_ref[...] = jnp.broadcast_to(theta[:, dim:dim + 1], (hid, LANES))
            for start, stop in spans:
                logits(par, coefs, start, stop)
            for t in range(tiles - 1):
                update(t)
        slopes()
        new = k - 1
        pairs = list(range(max(0, k - HIST), k))
        dots = [jnp.zeros((8, LANES), F32)] * (2 + 2 * len(pairs))

        def products(t):
            g = g8(g_ref[par, :, col(t)])
            y = g - g8(g_ref[1 - par, :, col(t)])
            y_ref[new % HIST, :, col(t)] = y.reshape(hid, LANES)
            ss = [g8(s_ref[i % HIST, :, col(t)]) for i in pairs]
            ys = [g8(y_ref[i % HIST, :, col(t)]) for i in pairs[:-1]] + [y]
            terms = [(ss[-1], g), (y, g)] + [(v, y) for v in ss] + [(v, y) for v in ys]
            dots[:] = [d + jnp.sum(a * b, axis=0) for d, (a, b) in zip(dots, terms)]

        gradient(k, par, reg, products)
        row = jnp.zeros((1, LANES), F32)
        for i, d in enumerate(dots):
            d = jnp.sum(jnp.sum(d, axis=0, keepdims=True), axis=1, keepdims=True)
            row = jnp.where(lane8[0:1] == i, d, row)
        dbuf[me] = row
        for d in order:
            dcopy(d).start()
        if k < NUM_ITERS - 1:
            pieces(g_ref.at[par])

            def multiply(c, carry):
                forward(k + 1, pl.ds(pl.multiple_of(c * per, per), per))
                return carry

            lax.fori_loop(0, CHUNKS, multiply, 0)
        sent(par)
        for d in order:
            darrive(d).wait_recv()
        total = dbuf[0]
        for i in range(1, n):
            total += dbuf[i]
        vals = [jnp.broadcast_to(total[:, i:i + 1], (8, LANES)) for i in range(len(dots))]
        for i, v in zip(pairs, vals[2:2 + len(pairs)]):
            sy[i, new] = v
        for i, v in zip(pairs, vals[2 + len(pairs):]):
            yy[i, new] = yy[new, i] = v
        for i in pairs[:-1]:
            sg[i] = sg[i] + sy[i, new]
            yg[i] = yg[i] + yy[i, new]
        sg[new], yg[new] = vals[0], vals[1]
        rho[new] = 1.0 / sy[new, new]
        gamma = sy[new, new] / yy[new, new]
        a, diff = {}, {}
        for i in reversed(pairs):
            v = sg[i]
            for j in range(i + 1, k):
                v = v - a[j] * sy[i, j]
            a[i] = rho[i] * v
        for i in pairs:
            v = yg[i]
            for j in reversed(pairs):
                v = v - a[j] * yy[i, j]
            v = gamma * v
            for j in pairs:
                if j < i:
                    v = v + diff[j] * sy[j, i]
            diff[i] = a[i] - rho[i] * v
        cg = -step * gamma
        cy = {i: -cg * a[i] for i in pairs}
        cs = {i: -step * diff[i] for i in pairs}

        def update(t, k=k, par=par, pairs=pairs, cg=cg, cy=cy, cs=cs):
            s = cg * g8(g_ref[par, :, col(t)])
            for i in pairs:
                s = s + cy[i] * g8(y_ref[i % HIST, :, col(t)])
                s = s + cs[i] * g8(s_ref[i % HIST, :, col(t)])
            s_ref[k % HIST, :, col(t)] = s.reshape(hid, LANES)
            theta[:, col(t)] = (g8(theta[:, col(t)]) + s).reshape(hid, LANES)

        update(tiles - 1)
        part = [None] * (k + 1)

        def plus(j, v):
            part[j] = v if part[j] is None else part[j] + v

        plus(k, cg)
        for i in pairs:
            plus(i + 1, cy[i])
            plus(i, -cy[i])
            for j, v in enumerate(sigma[i]):
                plus(j, cs[i] * v)
        sigma[k] = [jnp.zeros((8, LANES), F32) if v is None else v for v in part]
        coefs = [coefs[0]] + [
            (coefs[j + 1] if j + 1 < len(coefs) else 0.0) + sigma[k][j] for j in range(k + 1)
        ]
        for d in order:
            dcopy(d).wait_send()

    for t in range(tiles - 1):
        update(t)


def unpack(rows, theta, lacc, wnew_ref, wonew_ref, loss_ref):
    hid, dim = wnew_ref.shape
    wnew_ref[...] = theta[:, 0:dim]
    lane = lax.broadcasted_iota(jnp.int32, (hid, LANES), 1)
    sub = lax.broadcasted_iota(jnp.int32, (hid, LANES), 0)
    w2col = theta[:, dim:dim + 1]
    wonew_ref[...] = jnp.sum(jnp.where(lane == sub, w2col, 0.0), axis=0, keepdims=True)[:, 0:hid]
    row = jnp.zeros((1, LANES), F32)
    for k in range(NUM_ITERS):
        loss = jnp.sum(jnp.sum(lacc[k], axis=0, keepdims=True), axis=1, keepdims=True)
        row = jnp.where(lane[0:1] == k, loss, row)
    loss_ref[...] = row[:, 0:NUM_ITERS] / rows


def solution(mesh):
    n = mesh.shape["feat"]

    def local_solve(x, t, w, wo, reg, step):
        rows, dim = x.shape
        hid = w.shape[0]
        width = dim // LANES * LANES + LANES
        vmem = pl.BlockSpec(memory_space=pltpu.VMEM)
        big = (x.T, t.reshape(rows // LANES, LANES), w, wo.reshape(1, hid))
        hbm = pl.BlockSpec(memory_space=pltpu.HBM)
        smem = pl.BlockSpec(memory_space=pltpu.SMEM)
        theta, lacc = pl.pallas_call(
            functools.partial(kernel, n, rows, hid, dim, hid * n),
            out_shape=(
                jax.ShapeDtypeStruct((hid, width), F32),
                jax.ShapeDtypeStruct((NUM_ITERS, 8, LANES), F32),
            ),
            in_specs=[hbm] * 4 + [smem] * 2,
            out_specs=(vmem, vmem),
            scratch_shapes=[
                pltpu.VMEM((rows, dim // LANES * LANES), BF16),
                pltpu.VMEM((dim, rows), BF16),
                pltpu.VMEM((LANES, rows), BF16),
                pltpu.VMEM((rows // LANES, LANES), F32),
                pltpu.VMEM((hid, dim), F32),
                pltpu.VMEM((1, hid), F32),
                pltpu.VMEM((NUM_ITERS, hid, rows), F32),
                pltpu.VMEM((hid, rows), F32),
                pltpu.VMEM((hid, rows), F32),
                pltpu.VMEM((3 * hid, rows), BF16),
                pltpu.VMEM((3 * hid, dim // LANES * LANES), BF16),
                pltpu.VMEM((hid, LANES), BF16),
                pltpu.VMEM((3 * hid, dim // LANES * LANES), F32),
                pltpu.VMEM((hid, LANES), F32),
                pltpu.VMEM((2, hid, width), F32),
                pltpu.VMEM((HIST, hid, width), F32),
                pltpu.VMEM((HIST, hid, width), F32),
                pltpu.VMEM((hid, LANES), F32),
                pltpu.VMEM((2, n, rows // LANES, LANES), F32),
                pltpu.VMEM((rows // LANES, LANES), F32),
                pltpu.VMEM((n, 1, LANES), F32),
                pltpu.SemaphoreType.DMA((CHUNKS,)),
                pltpu.SemaphoreType.DMA((3,)),
                pltpu.SemaphoreType.DMA((len(SPLIT), n)),
                pltpu.SemaphoreType.DMA((2, len(SPLIT), n)),
                pltpu.SemaphoreType.DMA((n,)),
                pltpu.SemaphoreType.DMA((n,)),
            ],
            compiler_params=pltpu.CompilerParams(
                collective_id=0, has_side_effects=True, vmem_limit_bytes=VMEM_BYTES
            ),
        )(*(pltpu.with_memory_space_constraint(v, pltpu.HBM) for v in big), reg, step)
        wnew, wonew, losses = pl.pallas_call(
            functools.partial(unpack, rows),
            out_shape=(
                jax.ShapeDtypeStruct((hid, dim), F32),
                jax.ShapeDtypeStruct((1, hid), F32),
                jax.ShapeDtypeStruct((1, NUM_ITERS), F32),
            ),
            in_specs=[vmem, vmem],
            out_specs=(vmem,) * 3,
            compiler_params=pltpu.CompilerParams(vmem_limit_bytes=4 * 1024 * 1024),
        )(theta, lacc)
        return wnew, wonew.reshape(hid), losses.reshape(NUM_ITERS)

    specs_in = (P("prob", None), P("prob"), P(("prob", "feat"), None), P(("prob", "feat")), P("prob"), P("prob"))
    specs_out = (P(("prob", "feat"), None), P(("prob", "feat")), P("prob"))
    return jax.shard_map(local_solve, mesh=mesh, in_specs=specs_in, out_specs=specs_out, check_vma=False)
```

```python
import functools
import math

import jax
import jax.numpy as jnp
from jax import lax
from jax.experimental import pallas as pl
from jax.experimental.pallas import tpu as pltpu
from jax.sharding import PartitionSpec as P

NUM_ITERS = 6
HIST = 3
CHUNKS = 4
SPLIT = (1, 1, 2)
VMEM_BYTES = 50 * 1024 * 1024
LANES = 128
F32 = jnp.float32
BF16 = jnp.bfloat16
MESH = pl.DeviceIdType.MESH


def split3(v):
    hi = v.astype(BF16)
    rest = v - hi.astype(F32)
    mid = rest.astype(BF16)
    lo = (rest - mid.astype(F32)).astype(BF16)
    return hi, mid, lo


def kernel(
    n, rows, hid, dim, out_units,
    x_hbm, t_hbm, w_hbm, wo_hbm, reg_ref, step_ref,
    theta, lacc,
    xv, xr, xt, t_ref, w_ref, wo_ref, q_ref, h_ref, u_ref, d3_ref, g3_ref, gt_ref, acc_ref, tail_ref, g_ref,
    s_ref, y_ref, w2b_ref, zbuf, r_ref, dbuf,
    xsem, isem, zsend, zrecv, dsend, drecv,
):
    main = dim // LANES * LANES
    tail = dim - main
    width = main + LANES
    tiles = width // LANES
    groups = hid // 8
    per = rows // CHUNKS
    blocks = per // LANES
    sizes = [v * rows // (sum(SPLIT) * LANES) for v in SPLIT]
    spans = [(sum(sizes[:i]), sum(sizes[:i + 1])) for i in range(len(sizes))]
    in_scale = 1.0 / math.sqrt(dim)
    out_scale = 1.0 / math.sqrt(out_units)
    me = lax.axis_index("feat")

    def peer(d):
        return lax.rem(me + d, n)

    order = sorted(range(1, n), key=lambda d: -min(d, n - d))

    copies = [
        pltpu.make_async_copy(x_hbm.at[:, pl.ds(c * per, per)], xr.at[:, pl.ds(c * per, per)], xsem.at[c])
        for c in range(CHUNKS)
    ]
    inputs = [
        pltpu.make_async_copy(src, dst, isem.at[i])
        for i, (src, dst) in enumerate(
            ((w_hbm, w_ref), (wo_hbm, wo_ref), (t_hbm, t_ref)))
    ]
    for copy in inputs[:2] + copies + inputs[2:]:
        copy.start()
    barrier = pltpu.get_barrier_semaphore()
    for d in order:
        pl.semaphore_signal(barrier, inc=1, device_id={"feat": peer(d)}, device_id_type=MESH)

    lane8 = lax.broadcasted_iota(jnp.int32, (8, LANES), 1)
    lane = lax.broadcasted_iota(jnp.int32, (hid, LANES), 1)
    sub = lax.broadcasted_iota(jnp.int32, (hid, LANES), 0)

    def g8(v):
        return v.reshape(groups, 8, LANES)

    def col(t):
        return pl.ds(t * LANES, LANES)

    def pieces(src):
        for t in range(tiles - 1):
            for i, piece in enumerate(split3(src[:, col(t)])):
                g3_ref[i * hid:(i + 1) * hid, col(t)] = piece
        for i, piece in enumerate(split3(src[:, main:dim])):
            gt_ref[:, i * tail:(i + 1) * tail] = piece

    def forward(slot, rs):
        prod = jnp.dot(g3_ref[...], xr[0:main, rs], preferred_element_type=F32)
        prod_t = jnp.dot(gt_ref[...], xt[:, rs], preferred_element_type=F32)
        q_ref[slot, :, rs] = prod[0:hid] + (prod[hid:2 * hid] + (prod[2 * hid:3 * hid] + prod_t))

    def zcopy(par, c, d):
        return pltpu.make_async_remote_copy(
            src_ref=zbuf.at[par, me, pl.ds(spans[c][0], sizes[c])], dst_ref=zbuf.at[par, me, pl.ds(spans[c][0], sizes[c])],
            send_sem=zsend.at[c, d], recv_sem=zrecv.at[par, c, me],
            device_id={"feat": peer(d)}, device_id_type=MESH)

    def zarrive(par, c, d):
        source = peer(n - d)
        return pltpu.make_async_remote_copy(
            src_ref=zbuf.at[par, source, pl.ds(spans[c][0], sizes[c])],
            dst_ref=zbuf.at[par, source, pl.ds(spans[c][0], sizes[c])],
            send_sem=zsend.at[c, d], recv_sem=zrecv.at[par, c, source],
            device_id={"feat": source}, device_id_type=MESH)

    def dcopy(d):
        return pltpu.make_async_remote_copy(
            src_ref=dbuf.at[me], dst_ref=dbuf.at[me], send_sem=dsend.at[d], recv_sem=drecv.at[me],
            device_id={"feat": peer(d)}, device_id_type=MESH)

    def darrive(d):
        source = peer(n - d)
        return pltpu.make_async_remote_copy(
            src_ref=dbuf.at[source], dst_ref=dbuf.at[source], send_sem=dsend.at[d], recv_sem=drecv.at[source],
            device_id={"feat": source}, device_id_type=MESH)

    def logits(par, coefs, start, stop):
        scaled = [v * in_scale for v in coefs]
        for b in range(start, stop):
            cs = col(b)
            pre = scaled[0] * g8(q_ref[0, :, cs])
            for j in range(1, len(coefs)):
                pre += scaled[j] * g8(q_ref[j, :, cs])
            act = jnp.tanh(pre)
            h_ref[:, cs] = act.reshape(hid, LANES)
            part = jnp.sum(act * g8(w2b_ref[...]), axis=0)
            zbuf[par, me, b:b + 1, :] = jnp.sum(part, axis=0, keepdims=True) * out_scale
        for c, span in enumerate(spans):
            if start < span[1] <= stop:
                for d in order:
                    zcopy(par, c, d).start()

    def slopes():
        for b in range(rows // LANES):
            act = h_ref[:, col(b)]
            u_ref[:, col(b)] = w2b_ref[...] * (1.0 - act * act)

    def last_columns(rs):
        return lax.dot_general(
            xr[main:dim, rs], d3_ref[:, rs], (((1,), (1,)), ((), ())), preferred_element_type=F32)

    def gradient(it, par, reg, use):
        loss = jnp.zeros((8, LANES), F32)
        gw2 = jnp.zeros((groups, 8, LANES), F32)
        for c, (start, stop) in enumerate(spans):
            for d in order:
                zarrive(par, c, d).wait_recv()
            z = zbuf[par, 0, start:stop, :]
            for i in range(1, n):
                z += zbuf[par, i, start:stop, :]
            t = t_ref[start:stop, :]
            cost = jnp.maximum(z, 0.0) + jnp.log1p(jnp.exp(-jnp.abs(z))) - t * z
            loss += jnp.sum(cost.reshape((stop - start) // 8, 8, LANES), axis=0)
            r_ref[start:stop, :] = jax.nn.sigmoid(z) - t
            for i in range(start, stop):
                rrow = r_ref[i:i + 1, :]
                gw2 += g8(h_ref[:, col(i)] * rrow)
                for p, piece in enumerate(split3(u_ref[:, col(i)] * rrow)):
                    d3_ref[p * hid:(p + 1) * hid, col(i)] = piece
            rs = pl.ds(start * LANES, (stop - start) * LANES)
            if c < len(spans) - 1:
                prod = jnp.dot(d3_ref[:, rs], xv[rs, :], preferred_element_type=F32)
                sums = prod if c == 0 else sums + prod
                last = last_columns(rs) if c == 0 else last + last_columns(rs)
        lacc[it] = loss
        gw2 = jnp.sum(gw2.reshape(hid, LANES), axis=1, keepdims=True)
        rs = pl.ds(spans[-1][0] * LANES, sizes[-1] * LANES)
        def finish(t, total):
            g_ref[par, :, col(t)] = (g8(total) + reg * g8(theta[:, col(t)])).reshape(hid, LANES)
            use(t)

        scale = in_scale * out_scale / rows
        for start in range(0, main, 2 * LANES):
            cs = slice(start, start + 2 * LANES)
            prod = sums[:, cs] + jnp.dot(d3_ref[:, rs], xv[rs, cs], preferred_element_type=F32)
            prod = (prod[0:hid] + (prod[hid:2 * hid] + prod[2 * hid:3 * hid])) * scale
            finish(start // LANES, prod[:, :LANES])
            finish(start // LANES + 1, prod[:, LANES:])
            if start == 0:
                last = last + last_columns(rs)
                last = last[:, 0:hid] + (last[:, hid:2 * hid] + last[:, 2 * hid:3 * hid])
                tail_ref[:, 0:tail] = last.T * scale
                finish(tiles - 1, jnp.where(lane == tail, gw2 * (out_scale / rows), tail_ref[...]))

    def sent(par):
        for c in range(len(spans)):
            for d in order:
                zcopy(par, c, d).wait_send()

    def by_rows():
        def rows_of(c, carry):
            cs = pl.ds(pl.multiple_of(c * 2 * LANES, 2 * LANES), 2 * LANES)
            for t in range(tiles - 1):
                xv[cs, col(t)] = xr[col(t), cs].T
            return carry

        lax.fori_loop(0, rows // (2 * LANES), rows_of, 0)

    gt_ref[...] = jnp.zeros_like(gt_ref)
    tail_ref[...] = jnp.zeros_like(tail_ref)
    xt[3 * tail:, :] = jnp.zeros((LANES - 3 * tail, rows), BF16)
    for copy in inputs[:2]:
        copy.wait()
    w2col = jnp.sum(jnp.where(lane[:, :hid] == sub[:, :hid], wo_ref[...], 0.0), axis=1, keepdims=True)
    theta[:, main:width] = jnp.where(lane == tail, w2col, 0.0)
    theta[:, 0:main] = w_ref[:, 0:main]
    theta[:, main:dim] = w_ref[:, main:dim]
    w2b_ref[...] = jnp.broadcast_to(w2col, (hid, LANES))
    pieces(theta)
    pl.semaphore_wait(barrier, n - 1)

    one = jnp.ones((8, LANES), F32)
    for c in range(CHUNKS):
        rs = pl.ds(c * per, per)
        copies[c].wait()
        for i in range(3):
            xt[i * tail:(i + 1) * tail, rs] = xr[main:dim, rs]
        forward(0, rs)
        logits(0, [one], c * blocks, (c + 1) * blocks)
    for copy in inputs[2:]:
        copy.wait()
    reg = jnp.full((8, LANES), reg_ref[0], F32)
    step = jnp.full((8, LANES), step_ref[0], F32)
    slopes()
    by_rows()

    def first(t):
        s = -step * g8(g_ref[0, :, col(t)])
        s_ref[0, :, col(t)] = s.reshape(hid, LANES)
        theta[:, col(t)] = (g8(theta[:, col(t)]) + s).reshape(hid, LANES)

    gradient(0, 0, reg, first)
    pieces(g_ref.at[0])
    coefs = [one, -step]
    sigma = {0: [-step]}
    w2b_ref[...] = jnp.broadcast_to(theta[:, dim:dim + 1], (hid, LANES))
    for c in range(CHUNKS):
        rs = pl.ds(c * per, per)
        forward(1, rs)
        logits(1, coefs, c * blocks, (c + 1) * blocks)
    sent(0)

    rho, sy, yy, sg, yg = {}, {}, {}, {}, {}
    update = None
    for k in range(1, NUM_ITERS):
        par = k % 2
        if k > 1:
            w2b_ref[...] = jnp.broadcast_to(theta[:, dim:dim + 1], (hid, LANES))
            for start, stop in spans:
                logits(par, coefs, start, stop)
            for d in order:
                dcopy(d).wait_send()
            for t in range(tiles - 1):
                update(t)
        slopes()
        new = k - 1
        pairs = list(range(max(0, k - HIST), k))
        dots = [jnp.zeros((8, LANES), F32)] * (2 + 2 * len(pairs))

        def products(t):
            g = g8(g_ref[par, :, col(t)])
            y = g - g8(g_ref[1 - par, :, col(t)])
            y_ref[new % HIST, :, col(t)] = y.reshape(hid, LANES)
            ss = [g8(s_ref[i % HIST, :, col(t)]) for i in pairs]
            ys = [g8(y_ref[i % HIST, :, col(t)]) for i in pairs[:-1]] + [y]
            terms = [(ss[-1], g), (y, g)] + [(v, y) for v in ss] + [(v, y) for v in ys]
            dots[:] = [d + jnp.sum(a * b, axis=0) for d, (a, b) in zip(dots, terms)]

        gradient(k, par, reg, products)
        row = jnp.zeros((1, LANES), F32)
        for i, d in enumerate(dots):
            d = jnp.sum(jnp.sum(d, axis=0, keepdims=True), axis=1, keepdims=True)
            row = jnp.where(lane8[0:1] == i, d, row)
        dbuf[me] = row
        for d in order:
            dcopy(d).start()
        if k < NUM_ITERS - 1:
            pieces(g_ref.at[par])

            def multiply(c, carry):
                forward(k + 1, pl.ds(pl.multiple_of(c * per, per), per))
                return carry

            lax.fori_loop(0, CHUNKS, multiply, 0)
        sent(par)
        for d in order:
            darrive(d).wait_recv()
        total = dbuf[0]
        for i in range(1, n):
            total += dbuf[i]
        vals = [jnp.broadcast_to(total[:, i:i + 1], (8, LANES)) for i in range(len(dots))]
        for i, v in zip(pairs, vals[2:2 + len(pairs)]):
            sy[i, new] = v
        for i, v in zip(pairs, vals[2 + len(pairs):]):
            yy[i, new] = yy[new, i] = v
        for i in pairs[:-1]:
            sg[i] = sg[i] + sy[i, new]
            yg[i] = yg[i] + yy[i, new]
        sg[new], yg[new] = vals[0], vals[1]
        rho[new] = 1.0 / sy[new, new]
        gamma = sy[new, new] / yy[new, new]
        a, diff = {}, {}
        for i in reversed(pairs):
            v = sg[i]
            for j in range(i + 1, k):
                v = v - a[j] * sy[i, j]
            a[i] = rho[i] * v
        for i in pairs:
            v = yg[i]
            for j in reversed(pairs):
                v = v - a[j] * yy[i, j]
            v = gamma * v
            for j in pairs:
                if j < i:
                    v = v + diff[j] * sy[j, i]
            diff[i] = a[i] - rho[i] * v
        cg = -step * gamma
        cy = {i: -cg * a[i] for i in pairs}
        cs = {i: -step * diff[i] for i in pairs}

        def total_step(t, par=par, pairs=pairs, cg=cg, cy=cy, cs=cs):
            s = cg * g8(g_ref[par, :, col(t)])
            for i in pairs:
                s = s + cy[i] * g8(y_ref[i % HIST, :, col(t)])
                s = s + cs[i] * g8(s_ref[i % HIST, :, col(t)])
            return s

        def update(t, k=k, total_step=total_step):
            s = total_step(t)
            s_ref[k % HIST, :, col(t)] = s.reshape(hid, LANES)
            theta[:, col(t)] = (g8(theta[:, col(t)]) + s).reshape(hid, LANES)

        update(tiles - 1)
        part = [None] * (k + 1)

        def plus(j, v):
            part[j] = v if part[j] is None else part[j] + v

        plus(k, cg)
        for i in pairs:
            plus(i + 1, cy[i])
            plus(i, -cy[i])
            for j, v in enumerate(sigma[i]):
                plus(j, cs[i] * v)
        sigma[k] = [jnp.zeros((8, LANES), F32) if v is None else v for v in part]
        coefs = [coefs[0]] + [
            (coefs[j + 1] if j + 1 < len(coefs) else 0.0) + sigma[k][j] for j in range(k + 1)
        ]

    for t in range(tiles - 1):
        s = total_step(t)
        theta[:, col(t)] = (g8(theta[:, col(t)]) + s).reshape(hid, LANES)
    for d in order:
        dcopy(d).wait_send()


def unpack(rows, theta, lacc, wnew_ref, wonew_ref, loss_ref):
    hid, dim = wnew_ref.shape
    wnew_ref[...] = theta[:, 0:dim]
    lane = lax.broadcasted_iota(jnp.int32, (hid, LANES), 1)
    sub = lax.broadcasted_iota(jnp.int32, (hid, LANES), 0)
    w2col = theta[:, dim:dim + 1]
    wonew_ref[...] = jnp.sum(jnp.where(lane == sub, w2col, 0.0), axis=0, keepdims=True)[:, 0:hid]
    row = jnp.zeros((1, LANES), F32)
    for k in range(NUM_ITERS):
        loss = jnp.sum(jnp.sum(lacc[k], axis=0, keepdims=True), axis=1, keepdims=True)
        row = jnp.where(lane[0:1] == k, loss, row)
    loss_ref[...] = row[:, 0:NUM_ITERS] / rows


def solution(mesh):
    n = mesh.shape["feat"]

    def local_solve(x, t, w, wo, reg, step):
        rows, dim = x.shape
        hid = w.shape[0]
        width = dim // LANES * LANES + LANES
        vmem = pl.BlockSpec(memory_space=pltpu.VMEM)
        big = (x.T, t.reshape(rows // LANES, LANES), w, wo.reshape(1, hid))
        hbm = pl.BlockSpec(memory_space=pltpu.HBM)
        smem = pl.BlockSpec(memory_space=pltpu.SMEM)
        theta, lacc = pl.pallas_call(
            functools.partial(kernel, n, rows, hid, dim, hid * n),
            out_shape=(
                jax.ShapeDtypeStruct((hid, width), F32),
                jax.ShapeDtypeStruct((NUM_ITERS, 8, LANES), F32),
            ),
            in_specs=[hbm] * 4 + [smem] * 2,
            out_specs=(vmem, vmem),
            scratch_shapes=[
                pltpu.VMEM((rows, dim // LANES * LANES), BF16),
                pltpu.VMEM((dim, rows), BF16),
                pltpu.VMEM((LANES, rows), BF16),
                pltpu.VMEM((rows // LANES, LANES), F32),
                pltpu.VMEM((hid, dim), F32),
                pltpu.VMEM((1, hid), F32),
                pltpu.VMEM((NUM_ITERS, hid, rows), F32),
                pltpu.VMEM((hid, rows), F32),
                pltpu.VMEM((hid, rows), F32),
                pltpu.VMEM((3 * hid, rows), BF16),
                pltpu.VMEM((3 * hid, dim // LANES * LANES), BF16),
                pltpu.VMEM((hid, LANES), BF16),
                pltpu.VMEM((3 * hid, dim // LANES * LANES), F32),
                pltpu.VMEM((hid, LANES), F32),
                pltpu.VMEM((2, hid, width), F32),
                pltpu.VMEM((HIST, hid, width), F32),
                pltpu.VMEM((HIST, hid, width), F32),
                pltpu.VMEM((hid, LANES), F32),
                pltpu.VMEM((2, n, rows // LANES, LANES), F32),
                pltpu.VMEM((rows // LANES, LANES), F32),
                pltpu.VMEM((n, 1, LANES), F32),
                pltpu.SemaphoreType.DMA((CHUNKS,)),
                pltpu.SemaphoreType.DMA((3,)),
                pltpu.SemaphoreType.DMA((len(SPLIT), n)),
                pltpu.SemaphoreType.DMA((2, len(SPLIT), n)),
                pltpu.SemaphoreType.DMA((n,)),
                pltpu.SemaphoreType.DMA((n,)),
            ],
            compiler_params=pltpu.CompilerParams(
                collective_id=0, has_side_effects=True, vmem_limit_bytes=VMEM_BYTES
            ),
        )(*(pltpu.with_memory_space_constraint(v, pltpu.HBM) for v in big), reg, step)
        wnew, wonew, losses = pl.pallas_call(
            functools.partial(unpack, rows),
            out_shape=(
                jax.ShapeDtypeStruct((hid, dim), F32),
                jax.ShapeDtypeStruct((1, hid), F32),
                jax.ShapeDtypeStruct((1, NUM_ITERS), F32),
            ),
            in_specs=[vmem, vmem],
            out_specs=(vmem,) * 3,
            compiler_params=pltpu.CompilerParams(vmem_limit_bytes=4 * 1024 * 1024),
        )(theta, lacc)
        return wnew, wonew.reshape(hid), losses.reshape(NUM_ITERS)

    specs_in = (P("prob", None), P("prob"), P(("prob", "feat"), None), P(("prob", "feat")), P("prob"), P("prob"))
    specs_out = (P(("prob", "feat"), None), P(("prob", "feat")), P("prob"))
    return jax.shard_map(local_solve, mesh=mesh, in_specs=specs_in, out_specs=specs_out, check_vma=False)
```
